16 devices in a mesh: rep: 1, r: 2 (over z), s: 8 (over x, y, core).
Axes of the slice: x: 2, y: 2, z: 2, core: 2. Of those that a mesh axis runs over, the one named last changes fastest.
Arguments:
- x: bfloat16 [16, 2048, 1280], P(('rep', 'r', 's'))
- dy: bfloat16 [16, 2048, 1280], P(('rep', 'r', 's'))
- w_gate: bfloat16 [2, 1280, 4864], P(None, 's')
- w_up: bfloat16 [2, 1280, 4864], P(None, 's')
- w_down: bfloat16 [2, 4864, 1280], P(None, 's')
- m_w_gate: float32 [2, 1280, 4864], P(None, 's')
- m_w_up: float32 [2, 1280, 4864], P(None, 's')
- m_w_down: float32 [2, 4864, 1280], P(None, 's')
- v_w_gate: float32 [2, 1280, 4864], P(None, 's')
- v_w_up: float32 [2, 1280, 4864], P(None, 's')
- v_w_down: float32 [2, 4864, 1280], P(None, 's')
Outputs:
- output 1: bfloat16 [2, 1280, 4864], P('rep', 's')
- output 2: bfloat16 [2, 1280, 4864], P('rep', 's')
- output 3: bfloat16 [2, 4864, 1280], P('rep', 's')
- output 4: float32 [2, 1280, 4864], P('rep', 's')
- output 5: float32 [2, 1280, 4864], P('rep', 's')
- output 6: float32 [2, 4864, 1280], P('rep', 's')
- output 7: float32 [2, 1280, 4864], P('rep', 's')
- output 8: float32 [2, 1280, 4864], P('rep', 's')
- output 9: float32 [2, 4864, 1280], P('rep', 's')
All inputs are finite; a program needn't handle non-finite values.
Results may differ from the reference program's by a relative error of at most 0.0249.
Values are sent between devices in bfloat16 or wider.
A program may use at most 2 GiB of HBM per device.

```python
import jax
import jax.numpy as jnp
from jax import lax

SEQUENCES = 16
TOKENS = 2048
D = 1280
FF = 4864
LAYERS = 2
NAMES = ("w_gate", "w_up", "w_down")
SHAPES = {"w_gate": (LAYERS, D, FF), "w_up": (LAYERS, D, FF), "w_down": (LAYERS, FF, D)}


def bump(key, n, height):
    away = (jnp.arange(n, dtype=jnp.int32) - jax.random.randint(key, (), 0, n, jnp.int32)) % n
    return jnp.where(away < n // 8, height, 1.0)


def together(key, own, strength):
    shared = jax.random.normal(key, own.shape[1:], jnp.float32)
    return (own + strength * shared) * lax.rsqrt(1 + strength * strength)


def setup_inputs(seed: int = 0, part: int = 0) -> dict:
    kx, kdy, ka, kb, kz, kf, kh, kl, *keys = jax.random.split(jax.random.key(seed), 8 + 3 * len(NAMES))
    kx, kdy, ka, kb = (jax.random.fold_in(k, part) for k in (kx, kdy, ka, kb))
    kw, km, kv = (keys[i::3] for i in range(3))
    shape = (SEQUENCES, TOKENS, D)
    much_x, much_dy = jax.random.uniform(kz, (2,), jnp.float32, 0.0, 1.0)
    loud = 2.0 ** jax.random.uniform(jax.random.fold_in(kz, 1), (), jnp.float32, -1.0, 2.0)
    layers = 2.0 ** jax.random.uniform(kl, (LAYERS, 1, 1), jnp.float32, -1.0, 1.0)
    x = together(ka, jax.random.normal(kx, shape, jnp.float32), much_x) * bump(kf, D, 4.0)
    dy = together(kb, jax.random.normal(kdy, shape, jnp.float32), much_dy)
    drawn = {"x": x.astype(jnp.bfloat16), "dy": (loud * dy * (SEQUENCES * TOKENS) ** -0.5).astype(jnp.bfloat16)}
    for key, name in zip(kw, NAMES, strict=True):
        w = jax.random.normal(key, SHAPES[name], jnp.float32) * SHAPES[name][1] ** -0.5
        drawn[name] = (w * {"w_gate": 1.0, "w_up": bump(kh, FF, 4.0), "w_down": layers}[name]).astype(jnp.bfloat16)
    for key, name in zip(km, NAMES, strict=True):
        drawn[f"m_{name}"] = 0.1 * jax.random.normal(key, SHAPES[name], jnp.float32)
    for key, name in zip(kv, NAMES, strict=True):
        drawn[f"v_{name}"] = jax.random.uniform(key, SHAPES[name], jnp.float32, 0.005, 0.015)
    return drawn


def matmul(a, w):
    return jnp.dot(a, w, preferred_element_type=jnp.float32).astype(jnp.bfloat16)


def normed(h):
    wide = h.astype(jnp.float32)
    scale = lax.rsqrt(jnp.mean(wide**2, -1, keepdims=True) + 1e-6)
    return (wide * scale).astype(jnp.bfloat16)


def layer(h, w):
    a = normed(h)
    gate = jnp.dot(a, w["w_gate"], preferred_element_type=jnp.float32)
    up = jnp.dot(a, w["w_up"], preferred_element_type=jnp.float32)
    return h + matmul((jax.nn.silu(gate) * up).astype(jnp.bfloat16), w["w_down"])


def adamw(w, m, v, g):
    m = 0.9 * m + 0.1 * g
    v = 0.95 * v + 0.05 * g * g
    step = m * lax.rsqrt(v + 1e-8) + 0.1 * w
    return (w - 0.02 * step).astype(jnp.bfloat16), m, v


def stack(weights, h):
    return lax.scan(lambda h, w: (layer(h, w), None), h, weights)[0]


def reference(x, dy, w_gate, w_up, w_down, m_w_gate, m_w_up, m_w_down, v_w_gate, v_w_up, v_w_down):
    weights = dict(zip(NAMES, (w_gate, w_up, w_down), strict=True))

    def take(so_far, sequence):
        h, by_y = sequence
        _, back = jax.vjp(lambda w: stack(w, h), weights)
        return jax.tree.map(lambda total, term: total + term.astype(jnp.float32), so_far, back(by_y)[0]), None

    none_yet = {name: jnp.zeros(w.shape, jnp.float32) for name, w in weights.items()}
    by_weights, _ = lax.scan(take, none_yet, (x, dy))
    gradients = [by_weights[name].astype(jnp.bfloat16).astype(jnp.float32) for name in NAMES]
    new = [
        adamw(w.astype(jnp.float32), m, v, g)
        for w, m, v, g in zip((w_gate, w_up, w_down), (m_w_gate, m_w_up, m_w_down), (v_w_gate, v_w_up, v_w_down), gradients, strict=True)
    ]
    return tuple(one[which] for which in range(3) for one in new)
```

```python
import functools

import jax
import jax.numpy as jnp
from jax import lax
from jax.experimental import pallas as pl
from jax.experimental.pallas import tpu as pltpu
from jax.sharding import PartitionSpec as P

BF16, F32 = jnp.bfloat16, jnp.float32
LIMIT = 61 * 1024 * 1024
ANY = pl.BlockSpec(memory_space=pl.ANY)


def normed(h):
    wide = h.astype(jnp.float32)
    scale = lax.rsqrt(jnp.mean(wide**2, -1, keepdims=True) + 1e-6)
    return (wide * scale).astype(jnp.bfloat16)


def adamw(w, m, v, g):
    m = 0.9 * m + 0.1 * g
    v = 0.95 * v + 0.05 * g * g
    step = m * lax.rsqrt(v + 1e-8) + 0.1 * w
    return (w - 0.02 * step).astype(jnp.bfloat16), m, v


def wide(value):
    return value.astype(F32)


def narrow(value):
    return value.astype(BF16)


def place():
    me = lax.axis_index("s")
    return me // 4, (me // 2) % 2, me % 2


def index_of(*changed):
    x, y, c = place()
    x, y, c = (1 - v if k in changed else v for k, v in (("x", x), ("y", y), ("c", c)))
    return x * 4 + y * 2 + c


def square_of(*changed):
    x, y, _ = place()
    x, y = (1 - v if k in changed else v for k, v in (("x", x), ("y", y)))
    return x * 2 + y


def device(way):
    return {"r": 1 - lax.axis_index("r")} if way == "z" else {"s": index_of(way)}


class Sends:
    def __init__(self, send_sem, recv_sem):
        self.send_sem, self.recv_sem, self.made = send_sem, recv_sem, {}

    def copy(self, number, way, src, dst):
        return pltpu.make_async_remote_copy(
            src_ref=src, dst_ref=dst, send_sem=self.send_sem.at[number], recv_sem=self.recv_sem.at[number],
            device_id=device(way), device_id_type=pl.DeviceIdType.MESH,
        )


class Gather:
    ways, copies, stages = ("x", "y", "c"), 8, 2

    def __init__(self, block):
        self.operands = (block,)
        self.shapes = (jax.ShapeDtypeStruct((8,) + block.shape, block.dtype),)
        self.half = block.shape[0] // 2

    def parts(self, sends, ins, outs):
        (b,), (g,) = ins, outs
        h = self.half
        me, by_x, by_y, by_xy = index_of(), index_of("x"), index_of("y"), index_of("x", "y")
        low, high = pl.ds(0, h), pl.ds(h, h)
        return [
            sends.copy(0, "x", b, g.at[me]),
            sends.copy(1, "y", b, g.at[me]),
            sends.copy(2, "c", b, g.at[me]),
            sends.copy(3, "y", g.at[by_x, low], g.at[by_x, low]),
            sends.copy(4, "x", g.at[by_y, high], g.at[by_y, high]),
            sends.copy(5, "c", g.at[by_x], g.at[by_x]),
            sends.copy(6, "c", g.at[by_y], g.at[by_y]),
            sends.copy(7, "c", g.at[by_xy], g.at[by_xy]),
        ]

    def stage(self, number, sends, ins, outs, local):
        part = self.parts(sends, ins, outs)
        own = pltpu.make_async_copy(ins[0], outs[0].at[index_of()], local)
        if number == 0:
            own.start()
            for each in part[:3]:
                each.start()
        elif number == 1:
            part[0].wait_recv()
            part[1].wait_recv()
            for each in part[3:7]:
                each.start()
        else:
            part[3].wait_recv()
            part[4].wait_recv()
            part[7].start()
            own.wait()
            for each in (2, 5, 6, 7):
                part[each].wait_recv()
            for each in part:
                each.wait_send()


class Scatter1:
    ways, copies, stages = ("x", "y"), 4, 1

    def __init__(self, sums):
        self.operands = (sums,)
        self.half = sums.shape[1] // 2
        shape = jax.ShapeDtypeStruct((2, self.half) + sums.shape[2:], sums.dtype)
        self.shapes = (shape, shape)

    def parts(self, sends, ins, outs):
        (s,), (rx, ry) = ins, outs
        low, high = pl.ds(0, self.half), pl.ds(self.half, self.half)
        far = square_of("x", "y")
        return [
            sends.copy(0, "x", s.at[far, low], rx.at[1]),
            sends.copy(1, "y", s.at[far, high], ry.at[1]),
            sends.copy(2, "x", s.at[square_of("x"), low], rx.at[0]),
            sends.copy(3, "y", s.at[square_of("y"), high], ry.at[0]),
        ]

    def stage(self, number, sends, ins, outs, local):
        for each in self.parts(sends, ins, outs):
            each.start() if number == 0 else each.wait()


class Scatter2(Scatter1):
    ways, copies, stages = ("x", "y"), 2, 1

    def __init__(self, to_y, to_x):
        self.operands = (to_y, to_x)
        self.shapes = tuple(jax.ShapeDtypeStruct(t.shape, t.dtype) for t in (to_y, to_x))

    def parts(self, sends, ins, outs):
        return [sends.copy(0, "y", ins[0], outs[0]), sends.copy(1, "x", ins[1], outs[1])]


class Across(Scatter1):
    ways, copies, stages = ("z",), 1, 1

    def __init__(self, block):
        self.operands = (block,)
        self.shapes = (jax.ShapeDtypeStruct(block.shape, block.dtype),)

    def parts(self, sends, ins, outs):
        return [sends.copy(0, "z", ins[0], outs[0])]


class Line:
    def __init__(self):
        self.calls, self.last = 0, None

    def call(self, name, body, steps, operands, in_specs, shapes, out_specs, scratch=(), ways=(), tasks=(), flops=0):
        tasks = list(tasks)
        ways = tuple(sorted(set(ways).union(*(t.ways for t in tasks))))
        counts = [len(operands), sum(len(t.operands) for t in tasks), len(shapes), sum(len(t.shapes) for t in tasks), len(scratch)]

        def kernel(*refs):
            refs = list(refs)
            ins, task_ins, outs, task_outs, own = ([refs.pop(0) for _ in range(n)] for n in counts)
            i = pl.program_id(0)
            held = []
            for t in tasks:
                a, task_ins = task_ins[: len(t.operands)], task_ins[len(t.operands) :]
                b, task_outs = task_outs[: len(t.shapes)], task_outs[len(t.shapes) :]
                sems, refs = refs[:3], refs[3:]
                held.append((t, Sends(sems[0], sems[1]), a, b, sems[2]))

            if ways:
                @pl.when(i == 0)
                def _():
                    barrier = pltpu.get_barrier_semaphore()
                    for way in ways:
                        pl.semaphore_signal(barrier, inc=1, device_id=device(way), device_id_type=pl.DeviceIdType.MESH)
                    pl.semaphore_wait(barrier, len(ways))
                    for t, sends, a, b, local in held:
                        t.stage(0, sends, a, b, local)

            for t, sends, a, b, local in held:
                for number in range(1, t.stages):
                    @pl.when(i == (steps * number * 2) // (t.stages * 2 - 1))
                    def _():
                        t.stage(number, sends, a, b, local)

            if body is not None:
                body(i, ins, outs, own)

            if held:
                @pl.when(i == steps - 1)
                def _():
                    for t, sends, a, b, local in held:
                        t.stage(t.stages, sends, a, b, local)

        sems = []
        for t in tasks:
            sems += [pltpu.SemaphoreType.DMA((t.copies,)), pltpu.SemaphoreType.DMA((t.copies,)), pltpu.SemaphoreType.DMA]
        task_operands = tuple(o for t in tasks for o in t.operands)
        task_shapes = tuple(s for t in tasks for s in t.shapes)
        given = tuple(operands) + task_operands
        if self.last is not None:
            given, _ = lax.optimization_barrier((given, self.last))
        params = {"collective_id": self.calls, "has_side_effects": True} if ways else {}
        results = pl.pallas_call(
            kernel,
            grid=(steps,),
            out_shape=tuple(shapes) + task_shapes,
            in_specs=list(in_specs) + [ANY] * len(task_operands),
            out_specs=list(out_specs) + [ANY] * len(task_shapes),
            scratch_shapes=list(scratch) + sems,
            name=name,
            compiler_params=pltpu.CompilerParams(dimension_semantics=("arbitrary",), vmem_limit_bytes=LIMIT, **params),
            cost_estimate=pl.CostEstimate(flops=flops, bytes_accessed=0, transcendentals=0),
        )(*given)
        self.calls += 1
        self.last = results[0]
        own, rest = results[: len(shapes)], list(results[len(shapes) :])
        moved = [[rest.pop(0) for _ in t.shapes] for t in tasks]
        return own, moved


def shape(*dims, dtype=BF16):
    return jax.ShapeDtypeStruct(dims, dtype)


def held_block(dims):
    return pl.BlockSpec(dims, lambda i: (0,) * len(dims), pipeline_mode=pl.Buffered(1))


def dot(a, b, contract=(1, 0)):
    return lax.dot_general(a, b, (((contract[0],), (contract[1],)), ((), ())), preferred_element_type=F32)


WIDTH = 256
TALL = 256


def norm_call(line, h, tasks):
    t, d = h.shape

    def body(i, ins, outs, own):
        a = normed(ins[0][...])
        outs[0][...] = a
        outs[1][...] = a.T

    return line.call(
        "norm", body, t // TALL, (h,), [pl.BlockSpec((TALL, d), lambda i: (i, 0))], (shape(t, d), shape(d, t)),
        [pl.BlockSpec((TALL, d), lambda i: (i, 0)), pl.BlockSpec((d, TALL), lambda i: (0, i))], tasks=tasks,
    )


def gate_call(line, a, w, tasks):
    t, d = a.shape
    f = w.shape[1]

    def body(i, ins, outs, own):
        outs[0][...] = dot(ins[0][...], ins[1][...])

    return line.call(
        "gate", body, f // WIDTH, (a, w), [held_block((t, d)), pl.BlockSpec((d, WIDTH), lambda i: (0, i))],
        (shape(t, f, dtype=F32),), [pl.BlockSpec((t, WIDTH), lambda i: (0, i))], tasks=tasks, flops=2 * t * d * f,
    )


def up_call(line, a, w, gate, tasks):
    t, d = a.shape
    f = w.shape[1]
    tile = pl.BlockSpec((t, WIDTH), lambda i: (0, i))

    def body(i, ins, outs, own):
        up = dot(ins[0][...], ins[1][...])
        outs[0][...] = up
        act = narrow(jax.nn.silu(ins[2][...]) * up)
        outs[1][...] = act
        outs[2][...] = act.T

    return line.call(
        "up", body, f // WIDTH, (a, w, gate), [held_block((t, d)), pl.BlockSpec((d, WIDTH), lambda i: (0, i)), tile],
        (shape(t, f, dtype=F32), shape(t, f), shape(f, t)), [tile, tile, pl.BlockSpec((WIDTH, t), lambda i: (i, 0))],
        tasks=tasks, flops=2 * t * d * f,
    )


def down_call(line, act, w, h, tasks):
    t, f = act.shape
    d = w.shape[1]
    rows = lambda n: pl.BlockSpec((TALL, n), lambda i: (i, 0))

    def body(i, ins, outs, own):
        new = ins[2][...] + narrow(dot(ins[0][...], ins[1][...]))
        outs[0][...] = new
        a = normed(new)
        outs[1][...] = a
        outs[2][...] = a.T

    return line.call(
        "down", body, t // TALL, (act, w, h), [rows(f), held_block((f, d)), rows(d)], (shape(t, d), shape(t, d), shape(d, t)),
        [rows(d), rows(d), pl.BlockSpec((d, TALL), lambda i: (0, i))], tasks=tasks, flops=2 * t * d * f,
    )


def by_act_call(line, by_h, w, gate, up, tasks):
    t, d = by_h.shape
    f = w.shape[0]
    tile = pl.BlockSpec((t, WIDTH), lambda i: (0, i))

    def body(i, ins, outs, own):
        by_act = wide(narrow(dot(ins[0][...], ins[1][...], (1, 1))))
        gate = ins[2][...]
        share = jax.nn.sigmoid(gate)
        silu = gate * share
        outs[0][...] = narrow(by_act * ins[3][...] * (share + silu * (1 - share)))
        outs[1][...] = narrow(by_act * silu)

    return line.call(
        "by_act", body, f // WIDTH, (by_h, w, gate, up), [held_block((t, d)), pl.BlockSpec((WIDTH, d), lambda i: (i, 0)), tile, tile],
        (shape(t, f), shape(t, f)), [tile, tile], tasks=tasks, flops=2 * t * d * f,
    )


def by_a_call(line, by, w, before, tasks):
    t, f = by.shape
    d = w.shape[0]
    rows = lambda n: pl.BlockSpec((TALL, n), lambda i: (i, 0))
    more = () if before is None else (before,)

    def body(i, ins, outs, own):
        new = narrow(dot(ins[0][...], ins[1][...], (1, 1)))
        if more:
            new = narrow(wide(new) + wide(ins[2][...]))
        outs[0][...] = new

    return line.call(
        "by_a", body, t // TALL, (by, w) + more, [rows(f), held_block((d, f))] + [rows(d)] * len(more), (shape(t, d),), [rows(d)],
        tasks=tasks, flops=2 * t * d * f,
    )


def by_wide_call(line, a_t, by, tasks):
    d, t = a_t.shape
    f = by.shape[1]
    rows, tiles = d // 8, f // WIDTH

    def body(i, ins, outs, own):
        mine, theirs, send_sem, recv_sem = own
        c = place()[2]

        def sent(n):
            return pltpu.make_async_remote_copy(
                src_ref=mine.at[n % 3, 1 - c], dst_ref=theirs.at[n], send_sem=send_sem.at[n % 3], recv_sem=recv_sem.at[n],
                device_id=device("c"), device_id_type=pl.DeviceIdType.MESH,
            )

        @pl.when((i >= 1) & (i <= tiles))
        def _():
            sent(i - 1).start()

        @pl.when(i < tiles)
        def _():
            new = narrow(dot(ins[0][...], ins[1][...])).reshape(4, 2, rows, WIDTH)
            slot = i % 3
            mine[slot, 0] = new[:, 0]
            mine[slot, 1] = new[:, 1]

        @pl.when(i >= 2)
        def _():
            n = i - 2
            sent(n).wait()
            outs[0][...] = narrow(wide(mine[n % 3, c]) + wide(theirs[n]))

    return line.call(
        "by_wide", body, tiles + 2, (a_t, by), [held_block((d, t)), pl.BlockSpec((t, WIDTH), lambda i: (0, jnp.minimum(i, tiles - 1)))],
        (shape(4, rows, f),), [pl.BlockSpec((4, rows, WIDTH), lambda i: (0, 0, jnp.maximum(i - 2, 0)))],
        scratch=[
            pltpu.VMEM((3, 2, 4, rows, WIDTH), BF16), pltpu.VMEM((tiles, 4, rows, WIDTH), BF16),
            pltpu.SemaphoreType.DMA((3,)), pltpu.SemaphoreType.DMA((tiles,)),
        ],
        ways=("c",), tasks=tasks, flops=2 * t * d * f,
    )


def by_down_call(line, act_t, by_h, tasks):
    f, t = act_t.shape
    d = by_h.shape[1]
    rows = f // 8

    def block(i):
        c = place()[2]
        return (i % 4) * 2 + jnp.where(i < 4, 1 - c, c), 0

    def body(i, ins, outs, own):
        mine, theirs, send_sem, recv_sem = own

        def sent(n):
            return pltpu.make_async_remote_copy(
                src_ref=mine.at[n], dst_ref=theirs.at[n], send_sem=send_sem.at[n], recv_sem=recv_sem.at[n],
                device_id=device("c"), device_id_type=pl.DeviceIdType.MESH,
            )

        @pl.when((i >= 1) & (i <= 4))
        def _():
            sent(i - 1).start()

        @pl.when(i < 4)
        def _():
            mine[i] = narrow(dot(ins[0][...], ins[1][...]))

        @pl.when(i >= 4)
        def _():
            new = wide(narrow(dot(ins[0][...], ins[1][...])))
            sent(i - 4).wait()
            outs[0][0] = narrow(new + wide(theirs[i - 4]))

    return line.call(
        "by_down", body, 8, (act_t, by_h), [pl.BlockSpec((rows, t), block), held_block((t, d))],
        (shape(4, rows, d),), [pl.BlockSpec((1, rows, d), lambda i: (jnp.maximum(i - 4, 0), 0, 0))],
        scratch=[
            pltpu.VMEM((4, rows, d), BF16), pltpu.VMEM((4, rows, d), BF16),
            pltpu.SemaphoreType.DMA((4,)), pltpu.SemaphoreType.DMA((4,)),
        ],
        ways=("c",), tasks=tasks, flops=2 * t * d * f,
    )


def move_call(line, tasks):
    def body(i, ins, outs, own):
        outs[0][...] = jnp.zeros_like(outs[0])

    return line.call("move", body, 1, (), [], (shape(8, 128, dtype=F32),), [pl.BlockSpec((8, 128), lambda i: (0, 0))], tasks=tasks)[1]


def second(sums, rx, ry):
    half = sums.shape[1] // 2
    to_y = lax.dynamic_index_in_dim(sums, square_of("y"), 0, False)[:half]
    to_x = lax.dynamic_index_in_dim(sums, square_of("x"), 0, False)[half:]
    return narrow(wide(to_y) + wide(rx[1])), narrow(wide(to_x) + wide(ry[1]))


def whole_block(sums, rx, ry, ry2, rx2):
    half = sums.shape[1] // 2
    own = wide(lax.dynamic_index_in_dim(sums, square_of(), 0, False))
    low = own[:half] + wide(rx[0]) + wide(ry2)
    high = own[half:] + wide(ry[0]) + wide(rx2)
    return narrow(jnp.concatenate([low, high]))


def solution(mesh):
    def step(x, dy, *arrays):
        weights, m, v = (arrays[i : i + 3] for i in (0, 3, 6))
        (wg, wu, wd), line = weights, Line()
        flat = lambda g: g.reshape(-1, g.shape[-1])
        h0, dy = x[0], dy[0]

        (a0, a0t), [[g]] = norm_call(line, h0, [Gather(wg[0])])
        (gate0,), [[u]] = gate_call(line, a0, flat(g), [Gather(wu[0])])
        wg0 = flat(g)
        (up0, act0, act0t), [[d]] = up_call(line, a0, flat(u), gate0, [Gather(wd[0])])
        wu0, wd0 = flat(u), flat(d)
        (h1, a1, a1t), [[g]] = down_call(line, act0, wd0, h0, [Gather(wg[1])])
        wg1 = flat(g)
        (gate1,), [[u]] = gate_call(line, a1, wg1, [Gather(wu[1])])
        wu1 = flat(u)
        (up1, act1, act1t), [[d]] = up_call(line, a1, wu1, gate1, [Gather(wd[1])])
        wd1 = flat(d)

        (sd1,), _ = by_down_call(line, act1t, dy, [])
        (dg1, du1), [pd1] = by_act_call(line, dy, wd1, gate1, up1, [Scatter1(sd1)])
        (sg1,), [qd1] = by_wide_call(line, a1t, dg1, [Scatter2(*second(sd1, *pd1))])
        bd1 = whole_block(sd1, *pd1, *qd1)
        (su1,), [pg1, zd1] = by_wide_call(line, a1t, du1, [Scatter1(sg1), Across(bd1)])
        (da,), [qg1] = by_a_call(line, dg1, wg1, None, [Scatter2(*second(sg1, *pg1))])
        bg1 = whole_block(sg1, *pg1, *qg1)
        (da,), [pu1, zg1] = by_a_call(line, du1, wu1, da, [Scatter1(su1), Across(bg1)])
        by_h = dy + jax.vjp(normed, h1)[1](da)[0]
        (sd0,), [qu1] = by_down_call(line, act0t, by_h, [Scatter2(*second(su1, *pu1))])
        bu1 = whole_block(su1, *pu1, *qu1)
        (dg0, du0), [pd0, zu1] = by_act_call(line, by_h, wd0, gate0, up0, [Scatter1(sd0), Across(bu1)])
        (sg0,), [qd0] = by_wide_call(line, a0t, dg0, [Scatter2(*second(sd0, *pd0))])
        bd0 = whole_block(sd0, *pd0, *qd0)
        (su0,), [pg0, zd0] = by_wide_call(line, a0t, du0, [Scatter1(sg0), Across(bd0)])
        pu0, qg0 = move_call(line, [Scatter1(su0), Scatter2(*second(sg0, *pg0))])
        bg0 = whole_block(sg0, *pg0, *qg0)
        qu0, zg0 = move_call(line, [Scatter2(*second(su0, *pu0)), Across(bg0)])
        bu0 = whole_block(su0, *pu0, *qu0)
        [zu0] = move_call(line, [Across(bu0)])

        total = lambda b, z: wide(narrow(wide(b) + wide(z[0])))
        gradients = [
            jnp.stack([total(bg0, zg0), total(bg1, zg1)]),
            jnp.stack([total(bu0, zu0), total(bu1, zu1)]),
            jnp.stack([total(bd0, zd0), total(bd1, zd1)]),
        ]
        new = [adamw(wide(w), m, v, g) for w, m, v, g in zip(weights, m, v, gradients, strict=True)]
        return tuple(one[which] for which in range(3) for one in new)

    states, cut = P(("rep", "r", "s"), None, None), P(None, "s", None)
    return jax.shard_map(
        step,
        mesh=mesh,
        in_specs=(states, states) + (cut,) * 9,
        out_specs=(P("rep", "s", None),) * 9,
        check_vma=False,
    )
```

```python
import functools

import jax
import jax.numpy as jnp
from jax import lax
from jax.experimental import pallas as pl
from jax.experimental.pallas import tpu as pltpu
from jax.sharding import PartitionSpec as P

BF16, F32 = jnp.bfloat16, jnp.float32
LIMIT = 61 * 1024 * 1024
ANY = pl.BlockSpec(memory_space=pl.ANY)


def normed(h):
    wide = h.astype(jnp.float32)
    scale = lax.rsqrt(jnp.mean(wide**2, -1, keepdims=True) + 1e-6)
    return (wide * scale).astype(jnp.bfloat16)


def by_norm(h, by):
    h, by = h.astype(jnp.float32), by.astype(jnp.float32)
    scale = lax.rsqrt(jnp.mean(h**2, -1, keepdims=True) + 1e-6)
    return (by * scale - h * (scale**3 * jnp.mean(by * h, -1, keepdims=True))).astype(jnp.bfloat16)


def adamw(w, m, v, g):
    m = 0.9 * m + 0.1 * g
    v = 0.95 * v + 0.05 * g * g
    step = m * lax.rsqrt(v + 1e-8) + 0.1 * w
    return (w - 0.02 * step).astype(jnp.bfloat16), m, v


def wide(value):
    return value.astype(F32)


def narrow(value):
    return value.astype(BF16)


def place():
    me = lax.axis_index("s")
    return me // 4, (me // 2) % 2, me % 2


def index_of(*changed):
    x, y, c = place()
    x, y, c = (1 - v if k in changed else v for k, v in (("x", x), ("y", y), ("c", c)))
    return x * 4 + y * 2 + c


def square_of(*changed):
    x, y, _ = place()
    x, y = (1 - v if k in changed else v for k, v in (("x", x), ("y", y)))
    return x * 2 + y


def device(way):
    return {"r": 1 - lax.axis_index("r")} if way == "z" else {"s": index_of(way)}


class Sends:
    def __init__(self, send_sem, recv_sem, scratch):
        self.send_sem, self.recv_sem, self.scratch = send_sem, recv_sem, scratch

    def copy(self, number, way, src, dst):
        return pltpu.make_async_remote_copy(
            src_ref=src, dst_ref=dst, send_sem=self.send_sem.at[number], recv_sem=self.recv_sem.at[number],
            device_id=device(way), device_id_type=pl.DeviceIdType.MESH,
        )


class Gather1:
    ways, copies, when, alias, held, scratch = ("x", "y", "c"), 3, (), {}, True, ()

    def __init__(self, blocks, number):
        self.operands = (blocks,)
        self.spec = pl.BlockSpec((1,) + blocks.shape[1:], lambda i: (number, 0, 0), pipeline_mode=pl.Buffered(1))
        self.shapes = (jax.ShapeDtypeStruct((8,) + blocks.shape[1:], blocks.dtype),)
        self.quarter = blocks.shape[1] // 4

    def stage(self, number, sends, ins, outs, local):
        b, g = ins[0].at[0], outs[0]
        me, part = index_of(), pl.ds(lax.axis_index("r") * self.quarter, 3 * self.quarter)
        own = pltpu.make_async_copy(b, g.at[me], local)
        copies = [sends.copy(0, "x", b.at[part], g.at[me, part]), sends.copy(1, "y", b.at[part], g.at[me, part]), sends.copy(2, "c", b, g.at[me])]
        for each in copies + [own]:
            each.start() if number == 0 else each.wait()


class Gather2:
    ways, copies, when, alias = ("x", "y", "z", "c"), 11, (0.5,), {0: 0}
    held, scratch = False, ()

    def __init__(self, so_far):
        self.operands = (so_far,)
        self.shapes = (jax.ShapeDtypeStruct(so_far.shape, so_far.dtype),)
        self.quarter = so_far.shape[1] // 4

    def stage(self, number, sends, ins, outs, local):
        g, q, z = outs[0], self.quarter, lax.axis_index("r")
        by_x, by_y, far = index_of("x"), index_of("y"), index_of("x", "y")
        three, theirs, missing = pl.ds(z * q, 3 * q), pl.ds(z * 3 * q, q), pl.ds((1 - z) * 3 * q, q)
        first, second = pl.ds(z * 2 * q, q), pl.ds(z * 2 * q + q, q)
        near, other = pl.ds(z * 2 * q, 2 * q), pl.ds((1 - z) * 2 * q, 2 * q)
        copies = [
            ("y", by_x, first), ("x", by_y, second), ("z", by_x, theirs), ("z", by_y, theirs), ("c", by_x, three), ("c", by_y, three),
            ("z", far, near), ("c", far, near), ("c", by_x, missing), ("c", by_y, missing), ("c", far, other),
        ]
        part = [sends.copy(n, way, g.at[block, rows], g.at[block, rows]) for n, (way, block, rows) in enumerate(copies)]
        if number == 0:
            for each in part[:6]:
                each.start()
        elif number == 1:
            part[0].wait_recv()
            part[1].wait_recv()
            part[6].start()
            part[7].start()
        else:
            part[2].wait_recv()
            part[8].start()
            part[3].wait_recv()
            part[9].start()
            part[6].wait_recv()
            part[10].start()
            for each in (4, 5, 7, 8, 9, 10):
                part[each].wait_recv()
            for each in part:
                each.wait_send()


class Hops:
    when, alias, held = (), {}, False

    def __init__(self, *sent):
        self.ways, self.operands = zip(*sent)
        self.copies, self.scratch = len(sent), ()
        self.shapes = tuple(jax.ShapeDtypeStruct(v.shape, v.dtype) for v in self.operands)

    def stage(self, number, sends, ins, outs, local):
        for n, way in enumerate(self.ways):
            each = sends.copy(n, way, ins[n], outs[n])
            each.start() if number == 0 else each.wait()


class LastHops:
    ways, alias, held, start, piece = ("x", "y", "z"), {}, False, 8, 64

    def __init__(self, to_y, to_x, part):
        self.pieces = [(at, min(self.piece, part.shape[0] - at)) for at in range(0, part.shape[0], self.piece)]
        self.copies = 2 + len(self.pieces)
        self.when = tuple(range(self.start, self.start + 1 + len(self.pieces)))
        self.operands = (to_y, to_x, part)
        self.half = to_y.shape[0]
        self.shapes = (jax.ShapeDtypeStruct(part.shape, BF16),) * 2
        hop = pltpu.VMEM(to_y.shape, BF16)
        self.scratch = (hop, hop, pltpu.VMEM(part.shape, F32), pltpu.VMEM(part.shape, BF16), pltpu.SemaphoreType.DMA)

    def stage(self, number, sends, ins, outs, local):
        (to_y, to_x, part), (block, over), (*scratch, out_sem) = ins, outs, sends.scratch
        from_y, from_x, sums, total = scratch
        low, high = pl.ds(0, self.half), pl.ds(self.half, self.half)
        by_y, by_x = sends.copy(0, "y", to_y, from_y), sends.copy(1, "x", to_x, from_x)
        across = [sends.copy(2 + n, "z", total.at[pl.ds(*piece)], over.at[pl.ds(*piece)]) for n, piece in enumerate(self.pieces)]
        load, store = pltpu.make_async_copy(part, sums, local), pltpu.make_async_copy(total, block, out_sem)
        if number == 0:
            for each in (by_y, by_x, load):
                each.start()
        elif number == 1:
            for each in (by_y, by_x, load):
                each.wait()
            total[low] = narrow(sums[low] + wide(from_y[...]))
            total[high] = narrow(sums[high] + wide(from_x[...]))
        elif number < 2 + len(across):
            across[number - 2].start()
            if number == 2:
                store.start()
        else:
            for each in across + [store]:
                each.wait()


class Line:
    def __init__(self):
        self.calls, self.last = 0, None

    def call(self, name, body, steps, operands, in_specs, shapes, out_specs, scratch=(), ways=(), tasks=(), flops=0):
        tasks = list(tasks)
        ways = tuple(sorted(set(ways).union(*(t.ways for t in tasks))))
        counts = [len(operands), sum(len(t.operands) for t in tasks), len(shapes), sum(len(t.shapes) for t in tasks), len(scratch)]

        def kernel(*refs):
            refs = list(refs)
            ins, task_ins, outs, task_outs, own = ([refs.pop(0) for _ in range(n)] for n in counts)
            i = pl.program_id(0)
            held = []
            for t in tasks:
                a, task_ins = task_ins[: len(t.operands)], task_ins[len(t.operands) :]
                b, task_outs = task_outs[: len(t.shapes)], task_outs[len(t.shapes) :]
                sems, more, refs = refs[:3], refs[3 : 3 + len(t.scratch)], refs[3 + len(t.scratch) :]
                held.append((t, Sends(sems[0], sems[1], more), a, b, sems[2]))

            if ways:
                @pl.when(i == 0)
                def _():
                    barrier = pltpu.get_barrier_semaphore()
                    for way in ways:
                        pl.semaphore_signal(barrier, inc=1, device_id=device(way), device_id_type=pl.DeviceIdType.MESH)
                    pl.semaphore_wait(barrier, len(ways))
                    for t, sends, a, b, local in held:
                        t.stage(0, sends, a, b, local)

            for t, sends, a, b, local in held:
                for number, when in enumerate(t.when):
                    @pl.when(i == (when if isinstance(when, int) else int(steps * when)))
                    def _():
                        t.stage(number + 1, sends, a, b, local)

            if body is not None:
                body(i, ins, outs, own)

            if held:
                @pl.when(i == steps - 1)
                def _():
                    for t, sends, a, b, local in held:
                        t.stage(len(t.when) + 1, sends, a, b, local)

        sems = []
        for t in tasks:
            sems += [pltpu.SemaphoreType.DMA((t.copies,)), pltpu.SemaphoreType.DMA((t.copies,)), pltpu.SemaphoreType.DMA, *t.scratch]
        task_operands = tuple(o for t in tasks for o in t.operands)
        task_shapes = tuple(s for t in tasks for s in t.shapes)
        given = tuple(operands) + task_operands
        if self.last is not None:
            given, _ = lax.optimization_barrier((given, self.last))
        aliases, ins, outs = {}, len(operands), len(shapes)
        for t in tasks:
            aliases.update({ins + a: outs + b for a, b in t.alias.items()})
            ins, outs = ins + len(t.operands), outs + len(t.shapes)
        params = {"collective_id": self.calls, "has_side_effects": True} if ways else {}
        results = pl.pallas_call(
            kernel,
            grid=(steps,),
            out_shape=tuple(shapes) + task_shapes,
            in_specs=list(in_specs) + [t.spec if t.held else ANY for t in tasks for o in t.operands],
            out_specs=list(out_specs) + [ANY] * len(task_shapes),
            scratch_shapes=list(scratch) + sems,
            name=name,
            input_output_aliases=aliases,
            compiler_params=pltpu.CompilerParams(dimension_semantics=("arbitrary",), vmem_limit_bytes=LIMIT, **params),
            cost_estimate=pl.CostEstimate(flops=flops, bytes_accessed=0, transcendentals=0),
        )(*given)
        self.calls += 1
        self.last = results[0]
        own, rest = results[: len(shapes)], list(results[len(shapes) :])
        moved = [[rest.pop(0) for _ in t.shapes] for t in tasks]
        return own, moved


def shape(*dims, dtype=BF16):
    return jax.ShapeDtypeStruct(dims, dtype)


def held_block(dims):
    return pl.BlockSpec(dims, lambda i: (0,) * len(dims), pipeline_mode=pl.Buffered(1))


def dot(a, b, contract=(1, 0)):
    return lax.dot_general(a, b, (((contract[0],), (contract[1],)), ((), ())), preferred_element_type=F32)


WIDTH = 256
TALL = 256


def norm_call(line, h, tasks):
    t, d = h.shape

    def body(i, ins, outs, own):
        a = normed(ins[0][...])
        outs[0][...] = a
        outs[1][...] = a.T

    return line.call(
        "norm", body, t // TALL, (h,), [pl.BlockSpec((TALL, d), lambda i: (i, 0))], (shape(t, d), shape(d, t)),
        [pl.BlockSpec((TALL, d), lambda i: (i, 0)), pl.BlockSpec((d, TALL), lambda i: (0, i))], tasks=tasks,
    )


def gate_call(line, a, w, tasks):
    t, d = a.shape
    f = w.shape[1]

    def body(i, ins, outs, own):
        outs[0][...] = dot(ins[0][...], ins[1][...])

    return line.call(
        "gate", body, f // WIDTH, (a, w), [held_block((t, d)), pl.BlockSpec((d, WIDTH), lambda i: (0, i))],
        (shape(t, f, dtype=F32),), [pl.BlockSpec((t, WIDTH), lambda i: (0, i))], tasks=tasks, flops=2 * t * d * f,
    )


def up_call(line, a, w, gate, tasks):
    t, d = a.shape
    f = w.shape[1]
    rows = lambda n: pl.BlockSpec((TALL, n), lambda i: (i, 0))

    def body(i, ins, outs, own):
        for start in range(0, f, WIDTH):
            s = slice(start, start + WIDTH)
            up = dot(ins[0][...], ins[1][:, s])
            outs[0][:, s] = up
            act = narrow(jax.nn.silu(ins[2][:, s]) * up)
            outs[1][:, s] = act
            outs[2][s] = act.T

    return line.call(
        "up", body, t // TALL, (a, w, gate), [rows(d), held_block((d, f)), rows(f)],
        (shape(t, f, dtype=F32), shape(t, f), shape(f, t)), [rows(f), rows(f), pl.BlockSpec((f, TALL), lambda i: (0, i))],
        tasks=tasks, flops=2 * t * d * f,
    )


def down_call(line, act, w, h, tasks):
    t, f = act.shape
    d = w.shape[1]
    rows = lambda n: pl.BlockSpec((TALL, n), lambda i: (i, 0))

    def body(i, ins, outs, own):
        new = ins[2][...] + narrow(dot(ins[0][...], ins[1][...]))
        outs[0][...] = new
        a = normed(new)
        outs[1][...] = a
        outs[2][...] = a.T

    return line.call(
        "down", body, t // TALL, (act, w, h), [rows(f), held_block((f, d)), rows(d)], (shape(t, d), shape(t, d), shape(d, t)),
        [rows(d), rows(d), pl.BlockSpec((d, TALL), lambda i: (0, i))], tasks=tasks, flops=2 * t * d * f,
    )


def by_a_call(line, by, w, more, tasks):
    t, f = by.shape
    d = w.shape[0]
    rows = lambda n: pl.BlockSpec((TALL, n), lambda i: (i, 0))

    def body(i, ins, outs, own):
        new = narrow(dot(ins[0][...], ins[1][...], (1, 1)))
        if more:
            new = narrow(wide(new) + wide(ins[2][...]))
            new = ins[4][...] + by_norm(ins[3][...], new)
        outs[0][...] = new

    return line.call(
        "by_a", body, t // TALL, (by, w) + more, [rows(f), held_block((d, f))] + [rows(d)] * len(more), (shape(t, d),), [rows(d)],
        tasks=tasks, flops=2 * t * d * f,
    )


RING = 6
HOPS = 4


def by_hidden_call(line, by_h, w, gate, up, a_t, tasks, first):
    t, d = by_h.shape
    f = w.shape[0]
    rows, half, tiles, both = d // 8, d // 16, f // WIDTH, 2 * WIDTH
    last = tiles - 1
    tile = pl.BlockSpec((t, WIDTH), lambda i: (0, jnp.minimum(i, last)))
    hops = HOPS if first else 2
    at = lambda *dims: pl.BlockSpec(dims, lambda i: (0, jnp.maximum(i - 2 * hops, 0)))
    low, high = pl.ds(0, half), pl.ds(half, half)

    def body(i, ins, outs, own):
        by, mine, theirs, pair, rx, ry, to_y, to_x, ry2, rx2, block, over, *sems = own
        c, here, by_x, by_y, far = place()[2], square_of(), square_of("x"), square_of("y"), square_of("x", "y")

        def copies(hop, n):
            k = n % RING
            made = {
                0: lambda: [("c", mine.at[k, 1 - c], theirs.at[k])],
                1: lambda: [
                    ("x", pair.at[k, far, low], rx.at[k, 1]), ("y", pair.at[k, far, high], ry.at[k, 1]),
                    ("x", pair.at[k, by_x, low], rx.at[k, 0]), ("y", pair.at[k, by_y, high], ry.at[k, 0]),
                ],
                2: lambda: [("y", to_y.at[k], ry2.at[k]), ("x", to_x.at[k], rx2.at[k])],
                3: lambda: [("z", block.at[k], over.at[k])],
            }[hop]()
            return [
                pltpu.make_async_remote_copy(
                    src_ref=src, dst_ref=dst, send_sem=sems[2 * hop].at[k, p], recv_sem=sems[2 * hop + 1].at[k, p],
                    device_id=device(way), device_id_type=pl.DeviceIdType.MESH,
                )
                for p, (way, src, dst) in enumerate(made)
            ]

        for hop in reversed(range(hops)):
            n = i - 1 - 2 * hop

            @pl.when((n >= 0) & (n < tiles))
            def _():
                for each in copies(hop, n):
                    each.start()

        @pl.when(i < tiles)
        def _():
            for start in range(0, t, 256):
                s = slice(start, start + 256)
                by_act = wide(narrow(dot(ins[0][s], ins[1][...], (1, 1))))
                gate = ins[2][s]
                share = jax.nn.sigmoid(gate)
                silu = gate * share
                by_gate = narrow(by_act * ins[3][s] * (share + silu * (1 - share)))
                by_up = narrow(by_act * silu)
                by[s, :WIDTH] = by_gate
                by[s, WIDTH:] = by_up
                if not first:
                    outs[6][s] = by_gate
                    outs[7][s] = by_up
            new = narrow(dot(ins[4][...], by[...])).reshape(4, 2, rows, both)
            mine[i % RING, 0] = new[:, 0]
            mine[i % RING, 1] = new[:, 1]

        def arrived(hop, act):
            n = i - 2 - 2 * hop

            @pl.when((n >= 0) & (n < tiles))
            def _():
                for each in copies(hop, n):
                    each.wait()
                act(n % RING)

        def of_pair(k):
            pair[k] = narrow(wide(mine[k, c]) + wide(theirs[k]))

        def of_first(k):
            if not first:
                for m in (0, 1):
                    s = pl.ds(m * WIDTH, WIDTH)
                    outs[3 * m][...] = narrow(wide(pair[k, by_y, low, s]) + wide(rx[k, 1, :, s]))
                    outs[3 * m + 1][...] = narrow(wide(pair[k, by_x, high, s]) + wide(ry[k, 1, :, s]))
                    outs[3 * m + 2][low] = wide(pair[k, here, low, s]) + wide(rx[k, 0, :, s])
                    outs[3 * m + 2][high] = wide(pair[k, here, high, s]) + wide(ry[k, 0, :, s])
                return
            to_y[k] = narrow(wide(pair[k, by_y, low]) + wide(rx[k, 1]))
            to_x[k] = narrow(wide(pair[k, by_x, high]) + wide(ry[k, 1]))

        def of_second(k):
            block[k, low] = narrow(wide(pair[k, here, low]) + wide(rx[k, 0]) + wide(ry2[k]))
            block[k, high] = narrow(wide(pair[k, here, high]) + wide(ry[k, 0]) + wide(rx2[k]))

        def of_all(k):
            total = narrow(wide(block[k]) + wide(over[k]))
            outs[0][...] = total[:, :WIDTH]
            outs[1][...] = total[:, WIDTH:]

        for hop, act in enumerate((of_pair, of_first, of_second, of_all)[:hops]):
            arrived(hop, act)

    if first:
        shapes, out_specs = (shape(rows, f),) * 2, [at(rows, WIDTH)] * 2
    else:
        shapes = (shape(half, f), shape(half, f), shape(rows, f, dtype=F32)) * 2 + (shape(t, f),) * 2
        out_specs = [at(half, WIDTH), at(half, WIDTH), at(rows, WIDTH)] * 2 + [tile, tile]
    return line.call(
        "by_hidden", body, tiles + 2 * hops, (by_h, w, gate, up, a_t),
        [held_block((t, d)), pl.BlockSpec((WIDTH, d), lambda i: (jnp.minimum(i, last), 0)), tile, tile, held_block((d, t))],
        shapes, out_specs,
        scratch=[
            pltpu.VMEM((t, both), BF16),
            pltpu.VMEM((RING, 2, 4, rows, both), BF16), pltpu.VMEM((RING, 4, rows, both), BF16), pltpu.VMEM((RING, 4, rows, both), BF16),
            pltpu.VMEM((RING, 2, half, both), BF16), pltpu.VMEM((RING, 2, half, both), BF16),
            *[pltpu.VMEM((RING, half, both), BF16)] * 4, *[pltpu.VMEM((RING, rows, both), BF16)] * 2,
            *[pltpu.SemaphoreType.DMA((RING, n)) for n in (1, 1, 4, 4, 2, 2, 1, 1)],
        ],
        ways=("c", "x", "y", "z") if first else ("c", "x", "y"), tasks=tasks, flops=6 * t * d * f,
    )


def by_down_call(line, act_t, by_h, tasks):
    f, t = act_t.shape
    d = by_h.shape[1]
    rows = f // 8
    half = rows // 2
    low, high = pl.ds(0, half), pl.ds(half, half)

    def block(i):
        x, y, c = place()
        n = i // 2
        there_x = jnp.where(n % 2 == 0, jnp.where(n == 0, 1 - x, x), jnp.where(n == 1, 1 - x, x))
        there_y = jnp.where(n % 2 == 0, 1 - y, y)
        return (there_x * 2 + there_y) * 2 + jnp.where(i % 2 == 0, 1 - c, c), 0

    def body(i, ins, outs, own):
        mine, theirs, pair, send_sem, recv_sem, hop_send, hop_recv = own
        rx, ry = outs[1:]

        def remote(way, src, dst, send, recv):
            return pltpu.make_async_remote_copy(
                src_ref=src, dst_ref=dst, send_sem=send, recv_sem=recv, device_id=device(way), device_id_type=pl.DeviceIdType.MESH,
            )

        def sent(n):
            return remote("c", mine.at[n], theirs.at[n], send_sem.at[n], recv_sem.at[n])

        made = [("x", 0, low, rx.at[1]), ("y", 0, high, ry.at[1]), ("x", 1, low, rx.at[0]), ("y", 2, high, ry.at[0])]
        hop = [remote(way, pair.at[n, part], dst, hop_send.at[p], hop_recv.at[p]) for p, (way, n, part, dst) in enumerate(made)]

        @pl.when(i % 2 == 1)
        def _():
            sent(i // 2).start()

        for step, copies in ((2, hop[:2]), (4, hop[2:3]), (6, hop[3:])):
            @pl.when(i == step)
            def _():
                for each in copies:
                    each.start()

        @pl.when(i % 2 == 0)
        def _():
            mine[i // 2] = narrow(dot(ins[0][...], ins[1][...]))

        @pl.when(i % 2 == 1)
        def _():
            new = wide(narrow(dot(ins[0][...], ins[1][...])))
            n = i // 2
            sent(n).wait()
            total = narrow(new + wide(theirs[n]))
            pair[n] = total
            outs[0][0] = total

        @pl.when(i == 7)
        def _():
            for each in hop:
                each.wait()

    hopped = shape(2, half, d)
    return line.call(
        "by_down", body, 8, (act_t, by_h), [pl.BlockSpec((rows, t), block), held_block((t, d))],
        (shape(4, rows, d), hopped, hopped), [pl.BlockSpec((1, rows, d), lambda i: (i // 2, 0, 0)), ANY, ANY],
        scratch=[
            *[pltpu.VMEM((4, rows, d), BF16)] * 3,
            *[pltpu.SemaphoreType.DMA((4,))] * 4,
        ],
        ways=("c", "x", "y"), tasks=tasks, flops=2 * t * d * f,
    )


def move_call(line, tasks):
    def body(i, ins, outs, own):
        outs[0][...] = jnp.zeros_like(outs[0])

    return line.call("move", body, 1, (), [], (shape(8, 128, dtype=F32),), [pl.BlockSpec((8, 128), lambda i: (0, 0))], tasks=tasks)[1]


def second(sums, rx, ry):
    half = sums.shape[1] // 2
    to_y, to_x = wide(sums[2, :half]) + wide(rx[1]), wide(sums[1, half:]) + wide(ry[1])
    return narrow(to_y), narrow(to_x), wide(sums[3]) + wide(jnp.concatenate([rx[0], ry[0]]))


def solution(mesh):
    def step(x, dy, *arrays):
        weights, m, v = (arrays[i : i + 3] for i in (0, 3, 6))
        (wg, wu, wd), line = weights, Line()
        flat = lambda g: g.reshape(-1, g.shape[-1])
        h0, dy = x[0], dy[0]

        (a0, a0t), [[g]] = norm_call(line, h0, [Gather1(wg, 0)])
        [wg0], [u] = move_call(line, [Gather2(g), Gather1(wu, 0)])
        wg0 = flat(wg0)
        (gate0,), [[wu0], [d]] = gate_call(line, a0, wg0, [Gather2(u), Gather1(wd, 0)])
        wu0 = flat(wu0)
        (up0, act0, act0t), [[wd0], [g]] = up_call(line, a0, wu0, gate0, [Gather2(d), Gather1(wg, 1)])
        wd0 = flat(wd0)
        (h1, a1, a1t), [[wg1], [u]] = down_call(line, act0, wd0, h0, [Gather2(g), Gather1(wu, 1)])
        wg1 = flat(wg1)
        (gate1,), [[wu1], [d]] = gate_call(line, a1, wg1, [Gather2(u), Gather1(wd, 1)])
        wu1 = flat(wu1)
        (up1, act1, act1t), [[wd1]] = up_call(line, a1, wu1, gate1, [Gather2(d)])
        wd1 = flat(wd1)

        down1, _ = by_down_call(line, act1t, dy, [])
        to_y, to_x, part = second(*down1)
        (gy, gx, gpart, uy, ux, upart, dg1, du1), [(from_y, from_x)] = by_hidden_call(
            line, dy, wd1, gate1, up1, a1t, [Hops(("y", to_y), ("x", to_x))], False
        )
        joined = lambda part, from_y, from_x: narrow(part + wide(jnp.concatenate([from_y, from_x])))
        bd1 = joined(part, from_y, from_x)
        (da,), [(gfy, gfx, ufy, ufx), (zd1,)] = by_a_call(
            line, dg1, wg1, (), [Hops(("y", gy), ("x", gx), ("y", uy), ("x", ux)), Hops(("z", bd1))]
        )
        bg1, bu1 = joined(gpart, gfy, gfx), joined(upart, ufy, ufx)
        (by_h,), [(zg1,)] = by_a_call(line, du1, wu1, (da, h1, dy), [Hops(("z", bg1))])
        down0, [(zu1,)] = by_down_call(line, act0t, by_h, [Hops(("z", bu1))])
        (g0, u0), [(bd0, zd0)] = by_hidden_call(line, by_h, wd0, gate0, up0, a0t, [LastHops(*second(*down0))], True)

        total = lambda b, z: narrow(wide(b) + wide(z))
        gradients = [
            wide(jnp.stack(pair))
            for pair in ([g0, total(bg1, zg1)], [u0, total(bu1, zu1)], [total(bd0, zd0), total(bd1, zd1)])
        ]
        new = [adamw(wide(w), m, v, g) for w, m, v, g in zip(weights, m, v, gradients, strict=True)]
        return tuple(one[which] for which in range(3) for one in new)

    states, cut = P(("rep", "r", "s"), None, None), P(None, "s", None)
    return jax.shard_map(
        step,
        mesh=mesh,
        in_specs=(states, states) + (cut,) * 9,
        out_specs=(P("rep", "s", None),) * 9,
        check_vma=False,
    )
```

```python
import functools

import jax
import jax.numpy as jnp
from jax import lax
from jax.experimental import pallas as pl
from jax.experimental.pallas import tpu as pltpu
from jax.sharding import PartitionSpec as P

BF16, F32 = jnp.bfloat16, jnp.float32
LIMIT = 61 * 1024 * 1024
ANY = pl.BlockSpec(memory_space=pl.ANY)


def normed(h):
    wide = h.astype(jnp.float32)
    scale = lax.rsqrt(jnp.mean(wide**2, -1, keepdims=True) + 1e-6)
    return (wide * scale).astype(jnp.bfloat16)


def by_norm(h, by):
    h, by = h.astype(jnp.float32), by.astype(jnp.float32)
    scale = lax.rsqrt(jnp.mean(h**2, -1, keepdims=True) + 1e-6)
    return (by * scale - h * (scale**3 * jnp.mean(by * h, -1, keepdims=True))).astype(jnp.bfloat16)


def adamw(w, m, v, g):
    m = 0.9 * m + 0.1 * g
    v = 0.95 * v + 0.05 * g * g
    step = m * lax.rsqrt(v + 1e-8) + 0.1 * w
    return (w - 0.02 * step).astype(jnp.bfloat16), m, v


def wide(value):
    return value.astype(F32)


def narrow(value):
    return value.astype(BF16)


def place():
    me = lax.axis_index("s")
    return me // 4, (me // 2) % 2, me % 2


def index_of(*changed):
    x, y, c = place()
    x, y, c = (1 - v if k in changed else v for k, v in (("x", x), ("y", y), ("c", c)))
    return x * 4 + y * 2 + c


def square_of(*changed):
    x, y, _ = place()
    x, y = (1 - v if k in changed else v for k, v in (("x", x), ("y", y)))
    return x * 2 + y


def device(way):
    return {"r": 1 - lax.axis_index("r")} if way == "z" else {"s": index_of(way)}


class Sends:
    def __init__(self, send_sem, recv_sem, scratch):
        self.send_sem, self.recv_sem, self.scratch = send_sem, recv_sem, scratch

    def copy(self, number, way, src, dst):
        return pltpu.make_async_remote_copy(
            src_ref=src, dst_ref=dst, send_sem=self.send_sem.at[number], recv_sem=self.recv_sem.at[number],
            device_id=device(way), device_id_type=pl.DeviceIdType.MESH,
        )


class Gather1:
    ways, copies, when, alias, held, scratch = ("x", "y", "c"), 3, (), {}, True, ()

    def __init__(self, blocks, number):
        self.operands = (blocks,)
        self.spec = pl.BlockSpec((1,) + blocks.shape[1:], lambda i: (number, 0, 0), pipeline_mode=pl.Buffered(1))
        self.shapes = (jax.ShapeDtypeStruct((8,) + blocks.shape[1:], blocks.dtype),)
        self.quarter = blocks.shape[1] // 4

    def stage(self, number, sends, ins, outs, local):
        b, g = ins[0].at[0], outs[0]
        me, part = index_of(), pl.ds(lax.axis_index("r") * self.quarter, 3 * self.quarter)
        own = pltpu.make_async_copy(b, g.at[me], local)
        copies = [sends.copy(0, "x", b.at[part], g.at[me, part]), sends.copy(1, "y", b.at[part], g.at[me, part]), sends.copy(2, "c", b, g.at[me])]
        for each in copies + [own]:
            each.start() if number == 0 else each.wait()


class Gather2:
    ways, copies, when, alias = ("x", "y", "z", "c"), 11, (0.45,), {0: 0}
    held, scratch = False, ()

    def __init__(self, so_far):
        self.operands = (so_far,)
        self.shapes = (jax.ShapeDtypeStruct(so_far.shape, so_far.dtype),)
        self.quarter = so_far.shape[1] // 4

    def stage(self, number, sends, ins, outs, local):
        g, q, z = outs[0], self.quarter, lax.axis_index("r")
        by_x, by_y, far = index_of("x"), index_of("y"), index_of("x", "y")
        three, theirs, missing = pl.ds(z * q, 3 * q), pl.ds(z * 3 * q, q), pl.ds((1 - z) * 3 * q, q)
        first, second = pl.ds(z * 2 * q, q), pl.ds(z * 2 * q + q, q)
        near, other = pl.ds(z * 2 * q, 2 * q), pl.ds((1 - z) * 2 * q, 2 * q)
        copies = [
            ("y", by_x, first), ("x", by_y, second), ("z", by_x, theirs), ("z", by_y, theirs), ("c", by_x, three), ("c", by_y, three),
            ("z", far, near), ("c", far, near), ("c", by_x, missing), ("c", by_y, missing), ("c", far, other),
        ]
        part = [sends.copy(n, way, g.at[block, rows], g.at[block, rows]) for n, (way, block, rows) in enumerate(copies)]
        if number == 0:
            for each in part[:6]:
                each.start()
        elif number == 1:
            part[0].wait_recv()
            part[1].wait_recv()
            part[6].start()
            part[7].start()
        else:
            part[2].wait_recv()
            part[8].start()
            part[3].wait_recv()
            part[9].start()
            part[6].wait_recv()
            part[10].start()
            for each in (4, 5, 7, 8, 9, 10):
                part[each].wait_recv()
            for each in part:
                each.wait_send()


class Hops:
    when, alias, held = (), {}, False

    def __init__(self, *sent):
        self.ways, self.operands = zip(*sent)
        self.copies, self.scratch = len(sent), ()
        self.shapes = tuple(jax.ShapeDtypeStruct(v.shape, v.dtype) for v in self.operands)

    def stage(self, number, sends, ins, outs, local):
        for n, way in enumerate(self.ways):
            each = sends.copy(n, way, ins[n], outs[n])
            each.start() if number == 0 else each.wait()


class LastHops:
    ways, alias, held, start, piece = ("x", "y", "z"), {}, False, 5, 32

    def __init__(self, to_y, to_x, part):
        self.pieces = [(at, min(self.piece, part.shape[0] - at)) for at in range(0, part.shape[0], self.piece)]
        self.copies = 2 + len(self.pieces)
        self.when = tuple(range(self.start, self.start + 1 + len(self.pieces)))
        self.operands = (to_y, to_x, part)
        self.half = to_y.shape[0]
        self.shapes = (jax.ShapeDtypeStruct(part.shape, BF16),) * 2
        hop = pltpu.VMEM(to_y.shape, BF16)
        self.scratch = (hop, hop, pltpu.VMEM(part.shape, F32), pltpu.VMEM(part.shape, BF16), pltpu.SemaphoreType.DMA)

    def stage(self, number, sends, ins, outs, local):
        (to_y, to_x, part), (block, over), (*scratch, out_sem) = ins, outs, sends.scratch
        from_y, from_x, sums, total = scratch
        low, high = pl.ds(0, self.half), pl.ds(self.half, self.half)
        by_y, by_x = sends.copy(0, "y", to_y, from_y), sends.copy(1, "x", to_x, from_x)
        across = [sends.copy(2 + n, "z", total.at[pl.ds(*piece)], over.at[pl.ds(*piece)]) for n, piece in enumerate(self.pieces)]
        load, store = pltpu.make_async_copy(part, sums, local), pltpu.make_async_copy(total, block, out_sem)
        if number == 0:
            for each in (by_y, by_x, load):
                each.start()
        elif number == 1:
            for each in (by_y, by_x, load):
                each.wait()
            total[low] = narrow(sums[low] + wide(from_y[...]))
            total[high] = narrow(sums[high] + wide(from_x[...]))
        elif number < 2 + len(across):
            across[number - 2].start()
            if number == 2:
                store.start()
        else:
            for each in across + [store]:
                each.wait()


class Line:
    def __init__(self):
        self.calls, self.last = 0, None

    def call(self, name, body, steps, operands, in_specs, shapes, out_specs, scratch=(), ways=(), tasks=(), flops=0):
        tasks = list(tasks)
        ways = tuple(sorted(set(ways).union(*(t.ways for t in tasks))))
        resident = [n for n, spec in enumerate(in_specs) if isinstance(spec, Resident)]
        counts = [len(operands), sum(len(t.operands) for t in tasks), len(shapes), sum(len(t.shapes) for t in tasks), len(scratch)]

        def kernel(*refs):
            refs = list(refs)
            ins, task_ins, outs, task_outs, own = ([refs.pop(0) for _ in range(n)] for n in counts)
            i = pl.program_id(0)
            held, loads = [], []
            for n in resident:
                into, sem = refs.pop(0), refs.pop(0)
                loads.append(pltpu.make_async_copy(ins[n], into, sem))
                ins[n] = into

            if loads:
                @pl.when(i == 0)
                def _():
                    for each in loads:
                        each.start()

            for t in tasks:
                a, task_ins = task_ins[: len(t.operands)], task_ins[len(t.operands) :]
                b, task_outs = task_outs[: len(t.shapes)], task_outs[len(t.shapes) :]
                sems, more, refs = refs[:3], refs[3 : 3 + len(t.scratch)], refs[3 + len(t.scratch) :]
                held.append((t, Sends(sems[0], sems[1], more), a, b, sems[2]))

            if ways:
                @pl.when(i == 0)
                def _():
                    barrier = pltpu.get_barrier_semaphore()
                    for way in ways:
                        pl.semaphore_signal(barrier, inc=1, device_id=device(way), device_id_type=pl.DeviceIdType.MESH)
                    pl.semaphore_wait(barrier, len(ways))
                    for t, sends, a, b, local in held:
                        t.stage(0, sends, a, b, local)

            if loads:
                @pl.when(i == 0)
                def _():
                    for each in loads:
                        each.wait()

            for t, sends, a, b, local in held:
                for number, when in enumerate(t.when):
                    @pl.when(i == (when if isinstance(when, int) else int(steps * when)))
                    def _():
                        t.stage(number + 1, sends, a, b, local)

            if body is not None:
                body(i, ins, outs, own)

            if held:
                @pl.when(i == steps - 1)
                def _():
                    for t, sends, a, b, local in held:
                        t.stage(len(t.when) + 1, sends, a, b, local)

        sems = []
        for n in resident:
            sems += [pltpu.VMEM(in_specs[n].dims, operands[n].dtype), pltpu.SemaphoreType.DMA]
        for t in tasks:
            sems += [pltpu.SemaphoreType.DMA((t.copies,)), pltpu.SemaphoreType.DMA((t.copies,)), pltpu.SemaphoreType.DMA, *t.scratch]
        task_operands = tuple(o for t in tasks for o in t.operands)
        task_shapes = tuple(s for t in tasks for s in t.shapes)
        given = tuple(operands) + task_operands
        if self.last is not None:
            given, _ = lax.optimization_barrier((given, self.last))
        aliases, ins, outs = {}, len(operands), len(shapes)
        for t in tasks:
            aliases.update({ins + a: outs + b for a, b in t.alias.items()})
            ins, outs = ins + len(t.operands), outs + len(t.shapes)
        params = {"collective_id": self.calls, "has_side_effects": True} if ways else {}
        results = pl.pallas_call(
            kernel,
            grid=(steps,),
            out_shape=tuple(shapes) + task_shapes,
            in_specs=[ANY if isinstance(spec, Resident) else spec for spec in in_specs] + [t.spec if t.held else ANY for t in tasks for o in t.operands],
            out_specs=list(out_specs) + [ANY] * len(task_shapes),
            scratch_shapes=list(scratch) + sems,
            name=name,
            input_output_aliases=aliases,
            compiler_params=pltpu.CompilerParams(dimension_semantics=("arbitrary",), vmem_limit_bytes=LIMIT, **params),
            cost_estimate=pl.CostEstimate(flops=flops, bytes_accessed=0, transcendentals=0),
        )(*given)
        self.calls += 1
        self.last = results[0]
        own, rest = results[: len(shapes)], list(results[len(shapes) :])
        moved = [[rest.pop(0) for _ in t.shapes] for t in tasks]
        return own, moved


def shape(*dims, dtype=BF16):
    return jax.ShapeDtypeStruct(dims, dtype)


class Resident:
    def __init__(self, dims):
        self.dims = dims


def dot(a, b, contract=(1, 0)):
    return lax.dot_general(a, b, (((contract[0],), (contract[1],)), ((), ())), preferred_element_type=F32)


WIDTH = 256
TALL = 256


def norm_call(line, h, tasks):
    t, d = h.shape

    def body(i, ins, outs, own):
        a = normed(ins[0][...])
        outs[0][...] = a
        outs[1][...] = a.T

    return line.call(
        "norm", body, t // TALL, (h,), [pl.BlockSpec((TALL, d), lambda i: (i, 0))], (shape(t, d), shape(d, t)),
        [pl.BlockSpec((TALL, d), lambda i: (i, 0)), pl.BlockSpec((d, TALL), lambda i: (0, i))], tasks=tasks,
    )


def gate_call(line, a, w, tasks):
    t, d = a.shape
    f = w.shape[1]

    def body(i, ins, outs, own):
        outs[0][...] = dot(ins[0][...], ins[1][...])

    return line.call(
        "gate", body, f // WIDTH, (a, w), [Resident((t, d)), pl.BlockSpec((d, WIDTH), lambda i: (0, i))],
        (shape(t, f, dtype=F32),), [pl.BlockSpec((t, WIDTH), lambda i: (0, i))], tasks=tasks, flops=2 * t * d * f,
    )


def up_call(line, a, w, gate, tasks):
    t, d = a.shape
    f = w.shape[1]
    rows = lambda n: pl.BlockSpec((TALL, n), lambda i: (i, 0))

    def body(i, ins, outs, own):
        for start in range(0, f, WIDTH):
            s = slice(start, start + WIDTH)
            up = dot(ins[0][...], ins[1][:, s])
            outs[0][:, s] = up
            act = narrow(jax.nn.silu(ins[2][:, s]) * up)
            outs[1][:, s] = act
            outs[2][s] = act.T

    return line.call(
        "up", body, t // TALL, (a, w, gate),
        [rows(d), pl.BlockSpec((d, f), lambda i: (0, 0), pipeline_mode=pl.Buffered(1)), rows(f)],
        (shape(t, f, dtype=F32), shape(t, f), shape(f, t)), [rows(f), rows(f), pl.BlockSpec((f, TALL), lambda i: (0, i))],
        tasks=tasks, flops=2 * t * d * f,
    )


def down_call(line, act, w, h, tasks):
    t, f = act.shape
    d = w.shape[1]
    rows = lambda n: pl.BlockSpec((TALL, n), lambda i: (i, 0))

    def body(i, ins, outs, own):
        new = ins[2][...] + narrow(dot(ins[0][...], ins[1][...]))
        outs[0][...] = new
        a = normed(new)
        outs[1][...] = a
        outs[2][...] = a.T

    return line.call(
        "down", body, t // TALL, (act, w, h), [rows(f), Resident((f, d)), rows(d)], (shape(t, d), shape(t, d), shape(d, t)),
        [rows(d), rows(d), pl.BlockSpec((d, TALL), lambda i: (0, i))], tasks=tasks, flops=2 * t * d * f,
    )


def by_a_call(line, by, w, more, tasks):
    t, f = by.shape
    d = w.shape[0]
    rows = lambda n: pl.BlockSpec((TALL, n), lambda i: (i, 0))

    def body(i, ins, outs, own):
        new = narrow(dot(ins[0][...], ins[1][...], (1, 1)))
        if more:
            new = narrow(wide(new) + wide(ins[2][...]))
            new = ins[4][...] + by_norm(ins[3][...], new)
        outs[0][...] = new

    return line.call(
        "by_a", body, t // TALL, (by, w) + more, [rows(f), Resident((d, f))] + [rows(d)] * len(more), (shape(t, d),), [rows(d)],
        tasks=tasks, flops=2 * t * d * f,
    )


RING = 6
HOPS = 4


def by_hidden_call(line, by_h, w, gate, up, a_t, tasks, first):
    t, d = by_h.shape
    f = w.shape[0]
    rows, half, tiles, both = d // 8, d // 16, f // WIDTH, 2 * WIDTH
    last = tiles - 1
    tile = pl.BlockSpec((t, WIDTH), lambda i: (0, jnp.minimum(i, last)))
    hops = HOPS if first else 2
    at = lambda *dims: pl.BlockSpec(dims, lambda i: (0, jnp.maximum(i - 2 * hops, 0)))
    low, high = pl.ds(0, half), pl.ds(half, half)

    def body(i, ins, outs, own):
        by, mine, theirs, pair, rx, ry, to_y, to_x, ry2, rx2, block, over, *sems = own
        c, here, by_x, by_y, far = place()[2], square_of(), square_of("x"), square_of("y"), square_of("x", "y")

        def copies(hop, n):
            k = n % RING
            made = {
                0: lambda: [("c", mine.at[k, 1 - c], theirs.at[k])],
                1: lambda: [
                    ("x", pair.at[k, far, low], rx.at[k, 1]), ("y", pair.at[k, far, high], ry.at[k, 1]),
                    ("x", pair.at[k, by_x, low], rx.at[k, 0]), ("y", pair.at[k, by_y, high], ry.at[k, 0]),
                ],
                2: lambda: [("y", to_y.at[k], ry2.at[k]), ("x", to_x.at[k], rx2.at[k])],
                3: lambda: [("z", block.at[k], over.at[k])],
            }[hop]()
            return [
                pltpu.make_async_remote_copy(
                    src_ref=src, dst_ref=dst, send_sem=sems[2 * hop].at[k, p], recv_sem=sems[2 * hop + 1].at[k, p],
                    device_id=device(way), device_id_type=pl.DeviceIdType.MESH,
                )
                for p, (way, src, dst) in enumerate(made)
            ]

        for hop in reversed(range(hops)):
            n = i - 1 - 2 * hop

            @pl.when((n >= 0) & (n < tiles))
            def _():
                for each in copies(hop, n):
                    each.start()

        @pl.when(i < tiles)
        def _():
            for start in range(0, t, 256):
                s = slice(start, start + 256)
                by_act = wide(narrow(dot(ins[0][s], ins[1][...], (1, 1))))
                gate = ins[2][s]
                share = jax.nn.sigmoid(gate)
                silu = gate * share
                by_gate = narrow(by_act * ins[3][s] * (share + silu * (1 - share)))
                by_up = narrow(by_act * silu)
                by[s, :WIDTH] = by_gate
                by[s, WIDTH:] = by_up
                if not first:
                    outs[6][s] = by_gate
                    outs[7][s] = by_up
            new = narrow(dot(ins[4][...], by[...])).reshape(4, 2, rows, both)
            mine[i % RING, 0] = new[:, 0]
            mine[i % RING, 1] = new[:, 1]

        def arrived(hop, act):
            n = i - 2 - 2 * hop

            @pl.when((n >= 0) & (n < tiles))
            def _():
                for each in copies(hop, n):
                    each.wait()
                act(n % RING)

        def of_pair(k):
            pair[k] = narrow(wide(mine[k, c]) + wide(theirs[k]))

        def of_first(k):
            if not first:
                for m in (0, 1):
                    s = pl.ds(m * WIDTH, WIDTH)
                    outs[3 * m][...] = narrow(wide(pair[k, by_y, low, s]) + wide(rx[k, 1, :, s]))
                    outs[3 * m + 1][...] = narrow(wide(pair[k, by_x, high, s]) + wide(ry[k, 1, :, s]))
                    outs[3 * m + 2][low] = wide(pair[k, here, low, s]) + wide(rx[k, 0, :, s])
                    outs[3 * m + 2][high] = wide(pair[k, here, high, s]) + wide(ry[k, 0, :, s])
                return
            to_y[k] = narrow(wide(pair[k, by_y, low]) + wide(rx[k, 1]))
            to_x[k] = narrow(wide(pair[k, by_x, high]) + wide(ry[k, 1]))

        def of_second(k):
            block[k, low] = narrow(wide(pair[k, here, low]) + wide(rx[k, 0]) + wide(ry2[k]))
            block[k, high] = narrow(wide(pair[k, here, high]) + wide(ry[k, 0]) + wide(rx2[k]))

        def of_all(k):
            total = narrow(wide(block[k]) + wide(over[k]))
            outs[0][...] = total[:, :WIDTH]
            outs[1][...] = total[:, WIDTH:]

        for hop, act in enumerate((of_pair, of_first, of_second, of_all)[:hops]):
            arrived(hop, act)

    if first:
        shapes, out_specs = (shape(rows, f),) * 2, [at(rows, WIDTH)] * 2
    else:
        shapes = (shape(half, f), shape(half, f), shape(rows, f, dtype=F32)) * 2 + (shape(t, f),) * 2
        out_specs = [at(half, WIDTH), at(half, WIDTH), at(rows, WIDTH)] * 2 + [tile, tile]
    return line.call(
        "by_hidden", body, tiles + 2 * hops, (by_h, w, gate, up, a_t),
        [Resident((t, d)), pl.BlockSpec((WIDTH, d), lambda i: (jnp.minimum(i, last), 0)), tile, tile, Resident((d, t))],
        shapes, out_specs,
        scratch=[
            pltpu.VMEM((t, both), BF16),
            pltpu.VMEM((RING, 2, 4, rows, both), BF16), pltpu.VMEM((RING, 4, rows, both), BF16), pltpu.VMEM((RING, 4, rows, both), BF16),
            pltpu.VMEM((RING, 2, half, both), BF16), pltpu.VMEM((RING, 2, half, both), BF16),
            *[pltpu.VMEM((RING, half, both), BF16)] * 4, *[pltpu.VMEM((RING, rows, both), BF16)] * 2,
            *[pltpu.SemaphoreType.DMA((RING, n)) for n in (1, 1, 4, 4, 2, 2, 1, 1)],
        ],
        ways=("c", "x", "y", "z") if first else ("c", "x", "y"), tasks=tasks, flops=6 * t * d * f,
    )


def by_down_call(line, act_t, by_h, tasks):
    f, t = act_t.shape
    d = by_h.shape[1]
    rows = f // 8
    half = rows // 2
    low, high = pl.ds(0, half), pl.ds(half, half)

    def block(i):
        x, y, c = place()
        n = i // 2
        there_x = jnp.where(n % 2 == 0, jnp.where(n == 0, 1 - x, x), jnp.where(n == 1, 1 - x, x))
        there_y = jnp.where(n % 2 == 0, 1 - y, y)
        return (there_x * 2 + there_y) * 2 + jnp.where(i % 2 == 0, 1 - c, c), 0

    def body(i, ins, outs, own):
        mine, theirs, pair, rx, ry, send_sem, recv_sem, hop_send, hop_recv = own

        def remote(way, src, dst, send, recv):
            return pltpu.make_async_remote_copy(
                src_ref=src, dst_ref=dst, send_sem=send, recv_sem=recv, device_id=device(way), device_id_type=pl.DeviceIdType.MESH,
            )

        def sent(n):
            return remote("c", mine.at[n], theirs.at[n], send_sem.at[n], recv_sem.at[n])

        made = [("x", 0, low, rx.at[1]), ("y", 0, high, ry.at[1]), ("x", 1, low, rx.at[0]), ("y", 2, high, ry.at[0])]
        hop = [remote(way, pair.at[n, part], dst, hop_send.at[p], hop_recv.at[p]) for p, (way, n, part, dst) in enumerate(made)]

        @pl.when(i % 2 == 1)
        def _():
            sent(i // 2).start()

        for step, copies in ((2, hop[:2]), (4, hop[2:3]), (6, hop[3:])):
            @pl.when(i == step)
            def _():
                for each in copies:
                    each.start()

        @pl.when(i % 2 == 0)
        def _():
            mine[i // 2] = narrow(dot(ins[0][...], ins[1][...]))

        @pl.when(i % 2 == 1)
        def _():
            new = wide(narrow(dot(ins[0][...], ins[1][...])))
            n = i // 2
            sent(n).wait()
            total = narrow(new + wide(theirs[n]))
            pair[n] = total

        @pl.when(i == 7)
        def _():
            for each in hop:
                each.wait()
            outs[0][...] = narrow(wide(pair[2, low]) + wide(rx[1]))
            outs[1][...] = narrow(wide(pair[1, high]) + wide(ry[1]))
            outs[2][low] = wide(pair[3, low]) + wide(rx[0])
            outs[2][high] = wide(pair[3, high]) + wide(ry[0])

    whole = lambda n: pl.BlockSpec((n, d), lambda i: (0, 0))
    return line.call(
        "by_down", body, 8, (act_t, by_h), [pl.BlockSpec((rows, t), block), Resident((t, d))],
        (shape(half, d), shape(half, d), shape(rows, d, dtype=F32)), [whole(half), whole(half), whole(rows)],
        scratch=[
            *[pltpu.VMEM((4, rows, d), BF16)] * 3, *[pltpu.VMEM((2, half, d), BF16)] * 2,
            *[pltpu.SemaphoreType.DMA((4,))] * 4,
        ],
        ways=("c", "x", "y"), tasks=tasks, flops=2 * t * d * f,
    )


def move_call(line, tasks):
    def body(i, ins, outs, own):
        outs[0][...] = jnp.zeros_like(outs[0])

    return line.call("move", body, 1, (), [], (shape(8, 128, dtype=F32),), [pl.BlockSpec((8, 128), lambda i: (0, 0))], tasks=tasks)[1]


def solution(mesh):
    def step(x, dy, *arrays):
        weights, m, v = (arrays[i : i + 3] for i in (0, 3, 6))
        (wg, wu, wd), line = weights, Line()
        flat = lambda g: g.reshape(-1, g.shape[-1])
        h0, dy = x[0], dy[0]

        (a0, a0t), [[g]] = norm_call(line, h0, [Gather1(wg, 0)])
        [wg0], [u] = move_call(line, [Gather2(g), Gather1(wu, 0)])
        wg0 = flat(wg0)
        (gate0,), [[wu0], [d]] = gate_call(line, a0, wg0, [Gather2(u), Gather1(wd, 0)])
        wu0 = flat(wu0)
        (up0, act0, act0t), [[wd0], [g]] = up_call(line, a0, wu0, gate0, [Gather2(d), Gather1(wg, 1)])
        wd0 = flat(wd0)
        (h1, a1, a1t), [[wg1], [u]] = down_call(line, act0, wd0, h0, [Gather2(g), Gather1(wu, 1)])
        wg1 = flat(wg1)
        (gate1,), [[wu1], [d]] = gate_call(line, a1, wg1, [Gather2(u), Gather1(wd, 1)])
        wu1 = flat(wu1)
        (up1, act1, act1t), [[wd1]] = up_call(line, a1, wu1, gate1, [Gather2(d)])
        wd1 = flat(wd1)

        (to_y, to_x, part), _ = by_down_call(line, act1t, dy, [])
        (gy, gx, gpart, uy, ux, upart, dg1, du1), [(from_y, from_x)] = by_hidden_call(
            line, dy, wd1, gate1, up1, a1t, [Hops(("y", to_y), ("x", to_x))], False
        )
        joined = lambda part, from_y, from_x: narrow(part + wide(jnp.concatenate([from_y, from_x])))
        bd1 = joined(part, from_y, from_x)
        (da,), [(gfy, gfx, ufy, ufx), (zd1,)] = by_a_call(
            line, dg1, wg1, (), [Hops(("y", gy), ("x", gx), ("y", uy), ("x", ux)), Hops(("z", bd1))]
        )
        bg1, bu1 = joined(gpart, gfy, gfx), joined(upart, ufy, ufx)
        (by_h,), [(zg1,)] = by_a_call(line, du1, wu1, (da, h1, dy), [Hops(("z", bg1))])
        down0, [(zu1,)] = by_down_call(line, act0t, by_h, [Hops(("z", bu1))])
        (g0, u0), [(bd0, zd0)] = by_hidden_call(line, by_h, wd0, gate0, up0, a0t, [LastHops(*down0)], True)

        total = lambda b, z: narrow(wide(b) + wide(z))
        gradients = [
            wide(jnp.stack(pair))
            for pair in ([g0, total(bg1, zg1)], [u0, total(bu1, zu1)], [total(bd0, zd0), total(bd1, zd1)])
        ]
        new = [adamw(wide(w), m, v, g) for w, m, v, g in zip(weights, m, v, gradients, strict=True)]
        return tuple(one[which] for which in range(3) for one in new)

    states, cut = P(("rep", "r", "s"), None, None), P(None, "s", None)
    return jax.shard_map(
        step,
        mesh=mesh,
        in_specs=(states, states) + (cut,) * 9,
        out_specs=(P("rep", "s", None),) * 9,
        check_vma=False,
    )
```
